32 devices in a mesh: rep: 4 (over x, y), pp: 8 (over z, core).
Axes of the slice: x: 2, y: 2, z: 4, core: 2. Of those that a mesh axis runs over, the one named last changes fastest.
Arguments:
- x: bfloat16 [64, 512, 640], P('rep'), parts along dimension 0
- dy: bfloat16 [64, 512, 640], P('rep'), parts along dimension 0
- w_gate: bfloat16 [8, 640, 1536], P('pp')
- w_up: bfloat16 [8, 640, 1536], P('pp')
- w_down: bfloat16 [8, 1536, 640], P('pp')
Outputs:
- output 1: bfloat16 [32, 640, 1536], P(('rep', 'pp')), parts along dimension 0
- output 2: bfloat16 [32, 640, 1536], P(('rep', 'pp')), parts along dimension 0
- output 3: bfloat16 [32, 1536, 640], P(('rep', 'pp')), parts along dimension 0
There are 4 independent parts. The reference program is written for one: setup_inputs(seed, part) draws one part's arguments, and reference() takes and returns one part's arrays. A program takes and returns all parts, laid end to end along the dimension named above; an argument that names none is the same for every part.
All inputs are finite; a program needn't handle non-finite values.
Results may differ from the reference program's by a relative error of at most 0.0253.
Values are sent between devices in bfloat16 or wider.
A program may use at most 2 GiB of HBM per device.

```python
import jax
import jax.numpy as jnp
from jax import lax

MICRO = 16
TOKENS = 512
D = 640
FF = 1536
LAYERS = 8
NAMES = ("w_gate", "w_up", "w_down")
SHAPES = {"w_gate": (LAYERS, D, FF), "w_up": (LAYERS, D, FF), "w_down": (LAYERS, FF, D)}


def bump(key, n, height):
    away = (jnp.arange(n, dtype=jnp.int32) - jax.random.randint(key, (), 0, n, jnp.int32)) % n
    return jnp.where(away < n // 8, height, 1.0)


def together(key, own, strength):
    shared = jax.random.normal(key, own.shape[1:], jnp.float32)
    return (own + strength * shared) * lax.rsqrt(1 + strength * strength)


def setup_inputs(seed: int = 0, part: int = 0) -> dict:
    kx, kdy, ka, kb, kz, kf, kh, kl, *kw = jax.random.split(jax.random.key(seed), 8 + len(NAMES))
    kx, kdy, ka, kb = (jax.random.fold_in(k, part) for k in (kx, kdy, ka, kb))
    shape = (MICRO, TOKENS, D)
    much_x, much_dy = jax.random.uniform(kz, (2,), jnp.float32, 0.0, 1.0)
    layers = 2.0 ** jax.random.uniform(kl, (LAYERS, 1, 1), jnp.float32, -1.0, 1.0)
    x = together(ka, jax.random.normal(kx, shape, jnp.float32), much_x) * bump(kf, D, 4.0)
    dy = together(kb, jax.random.normal(kdy, shape, jnp.float32), much_dy)
    drawn = {"x": x.astype(jnp.bfloat16), "dy": (dy * (MICRO * TOKENS) ** -0.5).astype(jnp.bfloat16)}
    for key, name in zip(kw, NAMES, strict=True):
        w = jax.random.normal(key, SHAPES[name], jnp.float32) * SHAPES[name][1] ** -0.5
        drawn[name] = (w * {"w_gate": 1.0, "w_up": bump(kh, FF, 4.0), "w_down": layers}[name]).astype(jnp.bfloat16)
    return drawn


def matmul(a, w):
    return jnp.dot(a, w, preferred_element_type=jnp.float32).astype(jnp.bfloat16)


def normed(h):
    wide = h.astype(jnp.float32)
    scale = lax.rsqrt(jnp.mean(wide**2, -1, keepdims=True) + 1e-6)
    return (wide * scale).astype(jnp.bfloat16)


def layer(h, w):
    a = normed(h)
    gate = jnp.dot(a, w["w_gate"], preferred_element_type=jnp.float32)
    up = jnp.dot(a, w["w_up"], preferred_element_type=jnp.float32)
    return h + matmul((jax.nn.silu(gate) * up).astype(jnp.bfloat16), w["w_down"])


def stack(weights, h):
    return lax.scan(lambda h, w: (layer(h, w), None), h, weights)[0]


def reference(x, dy, w_gate, w_up, w_down):
    weights = dict(zip(NAMES, (w_gate, w_up, w_down), strict=True))

    def take(so_far, one):
        h, by_y = one
        _, back = jax.vjp(lambda w: stack(w, h), weights)
        return jax.tree.map(lambda total, term: total + term.astype(jnp.float32), so_far, back(by_y)[0]), None

    none_yet = {name: jnp.zeros(w.shape, jnp.float32) for name, w in weights.items()}
    by_weights, _ = lax.scan(take, none_yet, (x, dy))
    return tuple(by_weights[name].astype(jnp.bfloat16) for name in NAMES)
```

```python
import functools

import jax
import jax.numpy as jnp
from jax import lax
from jax.experimental import pallas as pl
from jax.experimental.pallas import tpu as pltpu
from jax.sharding import PartitionSpec as P

f32, bf16 = jnp.float32, jnp.bfloat16
MESH = pl.DeviceIdType.MESH
CHUNK = 256


def dot(a, b):
    return lax.dot_general(a, b, (((1,), (0,)), ((), ())), preferred_element_type=f32)


def dot_t(a, b):
    return lax.dot_general(a, b, (((1,), (1,)), ((), ())), preferred_element_type=f32)


def rounded(v):
    return v.astype(bf16).astype(f32)


def tiles(total, size):
    return [pl.ds(i, size) for i in range(0, total, size)]


def inverse_rms(h):
    return lax.rsqrt(jnp.mean(h * h, 0, keepdims=True) + 1e-6)


def transpose_into(dst, src, rows, cols):
    for r in tiles(rows, 128):
        for c in tiles(cols, 128):
            dst[c, r] = src[r, c].T


def f_norm(h, a, out):
    wide = h[...].astype(f32)
    a[...] = (wide * inverse_rms(wide)).astype(bf16)
    out[...] = h[...]


def f_up(w_gate, w_up, a, s_out, t_out, mid):
    for r in tiles(mid.shape[0], 256):
        g = dot(w_gate[r, :], a[...])
        u = dot(w_up[r, :], a[...])
        sig = 1.0 / (1.0 + jnp.exp(-g))
        s = g * sig
        s_out[r, :] = s
        t_out[r, :] = u * (sig + s * (1.0 - sig))
        mid[r, :] = (s * u).astype(bf16)


def f_down(w_down, mid, out):
    for r in tiles(out.shape[0], 320):
        o = rounded(dot(w_down[r, :], mid[...]))
        out[r, :] = (out[r, :].astype(f32) + o).astype(bf16)


def b_mid(w_down, dy, s_in, t_in, dg, du):
    for r in tiles(dg.shape[0], 256):
        dm = rounded(dot(w_down[r, :], dy[...]))
        dg[r, :] = (dm * t_in[r, :]).astype(bf16)
        du[r, :] = (dm * s_in[r, :]).astype(bf16)


def b_in(w_gate, w_up, dg, du, h, da):
    total = None
    for r in tiles(da.shape[0], 320):
        d = rounded(dot(w_gate[r, :], dg[...])) + rounded(dot(w_up[r, :], du[...]))
        d = d.astype(bf16)
        da[r, :] = d
        part = jnp.sum(d.astype(f32) * h[r, :].astype(f32), 0, keepdims=True)
        total = part if total is None else total + part
    return total


def b_norm(total, da, h, dy, out):
    wide = h[...].astype(f32)
    scale = inverse_rms(wide)
    k = scale * scale * scale * total * (1.0 / wide.shape[0])
    dh = rounded(da[...].astype(f32) * scale - wide * k)
    out[...] = (dy[...].astype(f32) + dh).astype(bf16)
    h[...] = (wide * scale).astype(bf16)


def kernel(stages, micro, x, dy, w_gate, w_up, w_down, o_gate, o_up, o_down, k_s, k_t, k_mid, k_dg, k_du,
           h_ring, y_ring, acc, st_s, st_t, dg, du, b_send, f_send, a_now, da, stage_in, wg, wu, wd,
           h_sem, y_sem, fs_sem, bs_sem, fo_sem, bi_sem, bo_sem, wi_sem, io_sem):
    me = lax.axis_index("pp")
    first, last = me == 0, me == stages - 1
    n = 2 * micro
    hidden = wd.shape[0]
    half = hidden // 2
    behind = stages - 1 - me
    lead = jnp.where(last, 1, jnp.minimum(4 * behind, n - 2))
    w_lag = jnp.where(lead > n - 5, 3, 0)

    barrier = pltpu.get_barrier_semaphore()

    @pl.when(me > 0)
    def _():
        pl.semaphore_signal(barrier, inc=1, device_id={"pp": me - 1}, device_id_type=MESH)

    @pl.when(me < stages - 1)
    def _():
        pl.semaphore_signal(barrier, inc=1, device_id={"pp": me + 1}, device_id_type=MESH)

    def load(src, c, slot):
        return pltpu.make_async_copy(src.at[c // 2, pl.ds((c % 2) * CHUNK, CHUNK), :], stage_in.at[slot], io_sem.at[slot])

    weights_in = [pltpu.make_async_copy(w.at[0], v, io_sem.at[2 + i]) for i, (w, v) in enumerate(((w_gate, wg), (w_up, wu), (w_down, wd)))]
    for copy in weights_in:
        copy.start()

    @pl.when(first)
    def _():
        load(x, 0, 0).start()
        load(x, 1, 1).start()

    @pl.when(last)
    def _():
        load(dy, 0, 0).start()
        load(dy, 1, 1).start()

    def send_f(c, slot):
        return pltpu.make_async_remote_copy(f_send.at[slot], h_ring.at[c], fs_sem.at[slot], h_sem.at[c], device_id={"pp": me + 1}, device_id_type=MESH)

    def send_b(c, slot):
        return pltpu.make_async_remote_copy(b_send.at[slot], y_ring.at[c], bs_sem.at[slot], y_sem.at[c], device_id={"pp": me - 1}, device_id_type=MESH)

    def keep_st(c):
        return [pltpu.make_async_copy(v.at[c % 2], k.at[c], fo_sem.at[i, c % 2]) for i, (v, k) in enumerate(((st_s, k_s), (st_t, k_t)))]

    def fetch_st(c):
        return [pltpu.make_async_copy(k.at[c], v.at[2 + c % 2], bi_sem.at[i, c % 2]) for i, (v, k) in enumerate(((st_s, k_s), (st_t, k_t)))]

    def keep_d(c):
        return [pltpu.make_async_copy(v.at[c % 2], k.at[c // 2, c % 2], bo_sem.at[i, c % 2]) for i, (v, k) in enumerate(((dg, k_dg), (du, k_du)))]

    def take_x(c):
        @pl.when(first & (c < n))
        def _():
            load(x, c, c % 2).wait()
            transpose_into(h_ring.at[c], stage_in.at[c % 2], CHUNK, wd.shape[1])

            @pl.when(c + 2 < n)
            def _():
                load(x, c + 2, c % 2).start()

    def forward_backward(fwd_refs, cf, cb):
        if cf is not None:
            wgt, wut, wdt, mid = fwd_refs

            def keep_mid(c):
                return pltpu.make_async_copy(mid.at[c % 2], k_mid.at[c // 2, c % 2], fo_sem.at[2, c % 2])

            @pl.when(me > 0)
            def _():
                send_f(cf, cf % 2).wait_recv()

            @pl.when(cf >= 2)
            def _():
                keep_mid(cf - 2).wait()

            @pl.when((cf >= 2) & (me < stages - 1))
            def _():
                send_f(cf - 2, cf % 2).wait_send()
                for copy in keep_st(cf - 2):
                    copy.wait()

        if cb is not None:

            @pl.when(me < stages - 1)
            def _():
                send_b(cb, cb % 2).wait_recv()
                for copy in fetch_st(cb):
                    copy.wait()

                @pl.when(cb + 1 < n)
                def _():
                    for copy in fetch_st(cb + 1):
                        copy.start()

            @pl.when(cb >= 2)
            def _():
                for copy in keep_d(cb - 2):
                    copy.wait()

            @pl.when((cb >= 2) & (me > 0))
            def _():
                send_b(cb - 2, cb % 2).wait_send()

            slot = jnp.where(last, cb % 2, 2 + cb % 2)
            b_mid(wd, y_ring.at[cb], st_s.at[slot], st_t.at[slot], dg.at[cb % 2], du.at[cb % 2])
        if cf is not None:
            f_norm(h_ring.at[cf], a_now, f_send.at[cf % 2])
            f_up(wgt, wut, a_now, st_s.at[cf % 2], st_t.at[cf % 2], mid.at[cf % 2])
        if cb is not None:
            total = b_in(wg, wu, dg.at[cb % 2], du.at[cb % 2], h_ring.at[cb], da)
        if cf is not None:
            f_down(wdt, mid.at[cf % 2], f_send.at[cf % 2])
        if cb is not None:
            b_norm(total, da, h_ring.at[cb], y_ring.at[cb], b_send.at[cb % 2])

        if cb is not None:

            @pl.when(me > 0)
            def _():
                send_b(cb, cb % 2).start()

            for copy in keep_d(cb):
                copy.start()
        if cf is not None:

            @pl.when(me < stages - 1)
            def _():
                send_f(cf, cf % 2).start()
                for copy in keep_st(cf):
                    copy.start()

            keep_mid(cf).start()

    def phase_f(wgt, wut, wdt, mid):
        refs = (wgt, wut, wdt, mid)
        for copy in weights_in:
            copy.wait()
        transpose_into(wgt, wg, *wg.shape)
        transpose_into(wut, wu, *wu.shape)
        transpose_into(wdt, wd, *wd.shape)
        take_x(0)
        pl.semaphore_wait(barrier, jnp.where(first | last, 1, 2))

        @pl.when(last)
        def _():
            def one(c, _):
                load(dy, c, c % 2).wait()
                transpose_into(y_ring.at[c], stage_in.at[c % 2], CHUNK, wd.shape[1])

                @pl.when(c + 2 < n)
                def _():
                    load(dy, c + 2, c % 2).start()

                return 0

            lax.fori_loop(0, n, one, 0)

        def only_f(c, _):
            forward_backward(refs, c, None)
            take_x(c + 1)
            return 0

        lax.fori_loop(0, lead, only_f, 0)
        for block in range(acc.shape[0]):
            acc[block] = jnp.zeros(acc.shape[1:], f32)

        @pl.when(me < stages - 1)
        def _():
            for copy in fetch_st(0):
                copy.start()

        def both(c, _):
            forward_backward(refs, lead + c, c)
            take_x(lead + c + 1)
            return 0

        lax.fori_loop(0, n - lead, both, 0)
        for c in (n - 2, n - 1):
            pltpu.make_async_copy(mid.at[c % 2], k_mid.at[c // 2, c % 2], fo_sem.at[2, c % 2]).wait()

            @pl.when(me < stages - 1)
            def _():
                send_f(c, c % 2).wait_send()
                for copy in keep_st(c):
                    copy.wait()

    rows, ff = w_gate.shape[1:]
    pl.run_scoped(
        phase_f, pltpu.VMEM((ff, rows), bf16), pltpu.VMEM((ff, rows), bf16), pltpu.VMEM((rows, ff), bf16), pltpu.VMEM((2, ff, CHUNK), bf16)
    )

    def phase_w(win):
        def fetch_w(w):
            return [
                pltpu.make_async_copy(k.at[w // 2, :, pl.ds((w % 2) * half, half), :], win.at[w % 3, i], wi_sem.at[w % 3, i])
                for i, k in enumerate((k_dg, k_du, k_mid))
            ]

        def half_w(w):
            for copy in fetch_w(w):
                copy.wait()

            @pl.when(w + 2 < n)
            def _():
                for copy in fetch_w(w + 2):
                    copy.start()

            c = (w // 2) * 2
            per = half // 256
            for i, left in enumerate((h_ring, h_ring, y_ring)):
                for j, r in enumerate(tiles(half, 256)):
                    term = dot_t(left[c], win[w % 3, i, 0, r, :]) + dot_t(left[c + 1], win[w % 3, i, 1, r, :])
                    block = i * 2 * per + (w % 2) * per + j
                    acc[block] += rounded(term)

        @pl.when(w_lag == 0)
        def _():
            for w in range(2):
                for copy in fetch_w(w):
                    copy.start()

        def b_and_w(j, _):
            forward_backward(None, None, n - lead + j)

            @pl.when((w_lag > 0) & (j == 1))
            def _():
                for copy in fetch_w(0):
                    copy.start()

            @pl.when((w_lag > 0) & (j == 2))
            def _():
                for copy in fetch_w(1):
                    copy.start()

            @pl.when(j >= w_lag)
            def _():
                half_w(j - w_lag)

            return 0

        lax.fori_loop(0, lead, b_and_w, 0)
        for c in (n - 2, n - 1):
            for copy in keep_d(c):
                copy.wait()

            @pl.when(me > 0)
            def _():
                send_b(c, c % 2).wait_send()

        def only_w(w, _):
            half_w(w)
            return 0

        lax.fori_loop(lead - w_lag, n, only_w, 0)

    pl.run_scoped(phase_w, pltpu.VMEM((3, 3, 2, half, CHUNK), bf16))
    per = 2 * half // 256
    outs = []
    for i, o in enumerate((o_gate, o_up, o_down)):
        for j, r in enumerate(tiles(hidden, 256)):
            h_ring[i * per + j] = acc[i * per + j].astype(bf16)
            outs.append(pltpu.make_async_copy(h_ring.at[i * per + j], o.at[0, :, r], io_sem.at[5 + i * per + j]))
            outs[-1].start()
    for copy in outs:
        copy.wait()


def solution(mesh):
    stages = mesh.shape["pp"]

    def step(x, dy, w_gate, w_up, w_down):
        micro, d = x.shape[0], x.shape[2]
        ff = w_gate.shape[2]
        n = 2 * micro
        hbm = pl.BlockSpec(memory_space=pltpu.HBM)
        out = jax.ShapeDtypeStruct((1, d, ff), bf16)
        kept = jax.ShapeDtypeStruct((n, ff, CHUNK), f32)
        paired = jax.ShapeDtypeStruct((micro, 2, ff, CHUNK), bf16)
        dma = pltpu.SemaphoreType.DMA
        d_gate, d_up, d_down, *_ = pl.pallas_call(
            functools.partial(kernel, stages, micro),
            out_shape=[out, out, out, kept, kept, paired, paired, paired],
            in_specs=[hbm] * 5,
            out_specs=[hbm] * 8,
            scratch_shapes=[
                pltpu.VMEM((n, d, CHUNK), bf16),
                pltpu.VMEM((n, d, CHUNK), bf16),
                pltpu.VMEM((3 * ff // 256, d, 256), f32),
                pltpu.VMEM((4, ff, CHUNK), f32),
                pltpu.VMEM((4, ff, CHUNK), f32),
                pltpu.VMEM((2, ff, CHUNK), bf16),
                pltpu.VMEM((2, ff, CHUNK), bf16),
                pltpu.VMEM((2, d, CHUNK), bf16),
                pltpu.VMEM((2, d, CHUNK), bf16),
                pltpu.VMEM((d, CHUNK), bf16),
                pltpu.VMEM((d, CHUNK), bf16),
                pltpu.VMEM((2, CHUNK, d), bf16),
                pltpu.VMEM((d, ff), bf16),
                pltpu.VMEM((d, ff), bf16),
                pltpu.VMEM((ff, d), bf16),
                dma((n,)),
                dma((n,)),
                dma((2,)),
                dma((2,)),
                dma((3, 2)),
                dma((2, 2)),
                dma((2, 2)),
                dma((3, 3)),
                dma((5 + 3 * ff // 256,)),
            ],
            compiler_params=pltpu.CompilerParams(collective_id=0, has_side_effects=True, vmem_limit_bytes=67043328),
        )(x, dy, w_gate, w_up, w_down)
        return d_gate, d_up, jnp.swapaxes(d_down, 1, 2)

    return jax.shard_map(
        step,
        mesh=mesh,
        in_specs=(P("rep", None, None),) * 2 + (P("pp", None, None),) * 3,
        out_specs=(P(("rep", "pp"), None, None),) * 3,
        check_vma=False,
    )
```

```python
import functools

import jax
import jax.numpy as jnp
from jax import lax
from jax.experimental import pallas as pl
from jax.experimental.pallas import tpu as pltpu
from jax.sharding import PartitionSpec as P

f32, bf16 = jnp.float32, jnp.bfloat16
MESH = pl.DeviceIdType.MESH
CHUNK = 256
SENDS = 4
SUB = 64
LEADS = (30, 27, 20, 17, 12, 9, 4, 1)


def dot(a, b):
    return lax.dot_general(a, b, (((1,), (0,)), ((), ())), preferred_element_type=f32)


def dot_t(a, b):
    return lax.dot_general(a, b, (((1,), (1,)), ((), ())), preferred_element_type=f32)


def rounded(v):
    return v.astype(bf16).astype(f32)


def tiles(total, size):
    return [pl.ds(i, size) for i in range(0, total, size)]


def inverse_rms(h):
    total = None
    for r in tiles(h.shape[0], SUB):
        wide = h[r, :].astype(f32)
        total = wide * wide if total is None else total + wide * wide
    return lax.rsqrt(jnp.sum(total, 0, keepdims=True) * (1.0 / h.shape[0]) + 1e-6)


def transpose_into(dst, src, rows, cols):
    for r in tiles(rows, 128):
        for c in tiles(cols, 128):
            dst[c, r] = src[r, c].T


def f_norm(h, a, out):
    scale = inverse_rms(h)
    for r in tiles(h.shape[0], SUB):
        a[r, :] = (h[r, :].astype(f32) * scale).astype(bf16)
        out[r, :] = h[r, :]


def f_up(w_gate, w_up, a, s_out, t_out, mid):
    for r in tiles(mid.shape[0], 256):
        g = dot(w_gate[r, :], a[...])
        u = dot(w_up[r, :], a[...])
        sig = 1.0 / (1.0 + jnp.exp(-g))
        s = g * sig
        s_out[r, :] = s
        t_out[r, :] = u * (sig + s * (1.0 - sig))
        mid[r, :] = (s * u).astype(bf16)


def f_down(w_down, mid, out):
    for r in tiles(out.shape[0], 320):
        out[r, :] += dot(w_down[r, :], mid[...]).astype(bf16)


def b_mid(w_down, dy, s_in, t_in, dg, du):
    for r in tiles(dg.shape[0], 256):
        dm = rounded(dot(w_down[r, :], dy[...]))
        dg[r, :] = (dm * t_in[r, :]).astype(bf16)
        du[r, :] = (dm * s_in[r, :]).astype(bf16)


def b_in(w_gate, w_up, dg, du, h, da):
    total = None
    for r in tiles(da.shape[0], 320):
        d = dot(w_gate[r, :], dg[...]).astype(bf16) + dot(w_up[r, :], du[...]).astype(bf16)
        da[r, :] = d
        part = d.astype(f32) * h[r, :].astype(f32)
        total = part if total is None else total + part
    return jnp.sum(total, 0, keepdims=True)


def b_norm(total, scale, h, dy, out):
    k = scale * scale * scale * total * (1.0 / h.shape[0])
    for q in tiles(h.shape[0], SUB):
        wide = h[q, :].astype(f32)
        dh = out[q, :].astype(f32) * scale - wide * k
        out[q, :] = dy[q, :] + dh.astype(bf16)
        h[q, :] = (wide * scale).astype(bf16)


def w_term(left, right):
    return dot_t(left[0], right[0]) + dot_t(left[1], right[1])


def w_add(acc, term):
    acc[...] += rounded(term)


def odd(i):
    return lax.rem(i, 2)


def half_of(i):
    return lax.div(i, 2)


def kernel(stages, micro, x, dy, w_gate, w_up, w_down, o_gate, o_up, o_down, k_s, k_t, k_mid, k_dg, k_du,
           h_ring, y_ring, dg, du, b_send, f_send, wg, wu, wd,
           h_sem, y_sem, fs_sem, bs_sem, fo_sem, bi_sem, bo_sem, wi_sem, io_sem):
    me = lax.axis_index("pp")
    first, last = me == 0, me == stages - 1
    n = 2 * micro
    hidden = wd.shape[0]
    half = hidden // 2
    lead = sum(jnp.where(me == s, v, 0) for s, v in enumerate(LEADS))
    w_lag = jnp.where(last, 0, jnp.where(lead > n - 5, 3, 1))
    rest = jnp.where(last, 0, lead)

    barrier = pltpu.get_barrier_semaphore()

    @pl.when(me > 0)
    def _():
        pl.semaphore_signal(barrier, inc=1, device_id={"pp": me - 1}, device_id_type=MESH)

    @pl.when(me < stages - 1)
    def _():
        pl.semaphore_signal(barrier, inc=1, device_id={"pp": me + 1}, device_id_type=MESH)

    weights_in = [pltpu.make_async_copy(w.at[0], v, io_sem.at[2 + i]) for i, (w, v) in enumerate(((w_gate, wg), (w_up, wu), (w_down, wd)))]
    for copy in weights_in:
        copy.start()

    def send_f(c):
        return pltpu.make_async_remote_copy(f_send.at[lax.rem(c, SENDS)], h_ring.at[c], fs_sem.at[lax.rem(c, SENDS)], h_sem.at[c], device_id={"pp": me + 1}, device_id_type=MESH)

    def send_b(c):
        return pltpu.make_async_remote_copy(b_send.at[lax.rem(c, SENDS)], y_ring.at[c], bs_sem.at[lax.rem(c, SENDS)], y_sem.at[c], device_id={"pp": me - 1}, device_id_type=MESH)

    def keep_st(st, c):
        return [pltpu.make_async_copy(v.at[odd(c)], k.at[c], fo_sem.at[i, odd(c)]) for i, (v, k) in enumerate(zip(st, (k_s, k_t)))]

    def fetch_st(st, hold, c):
        return [pltpu.make_async_copy(k.at[c], v.at[hold + odd(c)], bi_sem.at[i, odd(c)]) for i, (v, k) in enumerate(zip(st, (k_s, k_t)))]

    def keep_d(c):
        return [pltpu.make_async_copy(v.at[odd(c)], k.at[half_of(c), odd(c)], bo_sem.at[i, odd(c)]) for i, (v, k) in enumerate(((dg, k_dg), (du, k_du)))]

    def forward_backward(st, hold, until, cf, cb, fwd_refs=None, w=None, w_open=None, w_tiles=None):
        if cf is not None:
            wgt, wut, wdt, mid, a_now = fwd_refs

            def keep_mid(c):
                return pltpu.make_async_copy(mid.at[odd(c)], k_mid.at[half_of(c), odd(c)], fo_sem.at[2, odd(c)])

            @pl.when(me > 0)
            def _():
                with jax.named_scope("wait_h"):
                    send_f(cf).wait_recv()

            @pl.when(cf >= 2)
            def _():
                keep_mid(cf - 2).wait()

            @pl.when((cf >= 2) & (me < stages - 1))
            def _():
                for copy in keep_st(st, cf - 2):
                    copy.wait()

            @pl.when((cf >= SENDS) & (me < stages - 1))
            def _():
                with jax.named_scope("wait_fs"):
                    send_f(cf - SENDS).wait_send()

        if cb is not None:

            @pl.when(me < stages - 1)
            def _():
                with jax.named_scope("wait_y"):
                    send_b(cb).wait_recv()
                with jax.named_scope("wait_st"):
                    for copy in fetch_st(st, hold, cb):
                        copy.wait()

                @pl.when(cb + 1 < until)
                def _():
                    for copy in fetch_st(st, hold, cb + 1):
                        copy.start()

            @pl.when(cb >= 2)
            def _():
                with jax.named_scope("wait_d"):
                    for copy in keep_d(cb - 2):
                        copy.wait()

            @pl.when((cb >= SENDS) & (me > 0))
            def _():
                with jax.named_scope("wait_bs"):
                    send_b(cb - SENDS).wait_send()

        if w is not None:
            with jax.named_scope("wait_w"):
                w_open(w)
        with jax.named_scope(("F" if cf is not None else "") + ("B" if cb is not None else "") + ("W" if w is not None else "")):
            if cb is not None:
                slot, out = hold + odd(cb), b_send.at[lax.rem(cb, SENDS)]
                b_mid(wd, y_ring.at[cb], st[0].at[slot], st[1].at[slot], dg.at[odd(cb)], du.at[odd(cb)])
                scale = inverse_rms(h_ring.at[cb])
            if w is not None:
                for tile in w_tiles[: len(w_tiles) // 2]:
                    tile(w)
            if cf is not None:
                f_norm(h_ring.at[cf], a_now, f_send.at[lax.rem(cf, SENDS)])
                f_up(wgt, wut, a_now, st[0].at[odd(cf)], st[1].at[odd(cf)], mid.at[odd(cf)])
            if cb is not None:
                total = b_in(wg, wu, dg.at[odd(cb)], du.at[odd(cb)], h_ring.at[cb], out)
            if cf is not None:
                f_down(wdt, mid.at[odd(cf)], f_send.at[lax.rem(cf, SENDS)])
            if w is not None:
                for tile in w_tiles[len(w_tiles) // 2 :]:
                    tile(w)
            if cb is not None:
                b_norm(total, scale, h_ring.at[cb], y_ring.at[cb], out)

        if cb is not None:

            @pl.when(me > 0)
            def _():
                send_b(cb).start()

        if cf is not None:

            @pl.when(me < stages - 1)
            def _():
                send_f(cf).start()
                for copy in keep_st(st, cf):
                    copy.start()

            keep_mid(cf).start()
        if cb is not None:
            for copy in keep_d(cb):
                copy.start()

    def phase_f(st_s, st_t, wgt, wut, wdt, mid, a_now, stage_in):
        def load(src, c, slot):
            return pltpu.make_async_copy(src.at[half_of(c), pl.ds(odd(c) * CHUNK, CHUNK), :], stage_in.at[slot], io_sem.at[slot])

        def take_x(c):
            @pl.when(first & (c < n))
            def _():
                load(x, c, odd(c)).wait()
                transpose_into(h_ring.at[c], stage_in.at[odd(c)], CHUNK, wd.shape[1])

                @pl.when(c + 2 < n)
                def _():
                    load(x, c + 2, odd(c)).start()

        @pl.when(first)
        def _():
            load(x, 0, 0).start()
            load(x, 1, 1).start()

        @pl.when(last)
        def _():
            load(dy, 0, 0).start()
            load(dy, 1, 1).start()

        refs = (wgt, wut, wdt, mid, a_now)
        st = (st_s, st_t)
        hold = jnp.where(last, 0, 2)

        for copy, turned, w in zip(weights_in, (wgt, wut, wdt), (wg, wu, wd), strict=True):
            copy.wait()
            transpose_into(turned, w, *w.shape)
        take_x(0)
        pl.semaphore_wait(barrier, jnp.where(first | last, 1, 2))

        @pl.when(last)
        def _():
            def one(c, _):
                load(dy, c, odd(c)).wait()
                transpose_into(y_ring.at[c], stage_in.at[odd(c)], CHUNK, wd.shape[1])

                @pl.when(c + 2 < n)
                def _():
                    load(dy, c + 2, odd(c)).start()

                return 0

            lax.fori_loop(0, n, one, 0)

        def only_f(c, _):
            forward_backward(st, hold, n, c, None, refs)

            @pl.when((c == 2) & (me < stages - 1))
            def _():
                for copy in fetch_st(st, hold, 0):
                    copy.start()

            take_x(c + 1)
            return 0

        lax.fori_loop(0, lead, only_f, 0)

        def both(c, _):
            forward_backward(st, hold, n - lead, lead + c, c, refs)
            take_x(lead + c + 1)
            return 0

        lax.fori_loop(0, n - lead, both, 0)

        def only_b(c, _):
            forward_backward(st, hold, n, None, c)
            return 0

        lax.fori_loop(n - lead, n - rest, only_b, 0)
        for c in (n - 2, n - 1):
            pltpu.make_async_copy(mid.at[odd(c)], k_mid.at[half_of(c), odd(c)], fo_sem.at[2, odd(c)]).wait()

            @pl.when(me < stages - 1)
            def _():
                for copy in keep_st(st, c):
                    copy.wait()

    rows, ff = w_gate.shape[1:]
    shapes = (ff, rows), (ff, rows), (rows, ff), (2, ff, CHUNK), (rows, CHUNK), (2, CHUNK, rows)
    wide = pltpu.VMEM((4, ff, CHUNK), f32)
    pl.run_scoped(phase_f, wide, wide, *(pltpu.VMEM(shape, bf16) for shape in shapes))
    per = hidden // 256

    def phase_w(st_s, st_t, acc, win):
        st = (st_s, st_t)

        def fetch_w(w):
            return [
                pltpu.make_async_copy(k.at[half_of(w), :, pl.ds((odd(w)) * half, half), :], win.at[lax.rem(w, 4), i], wi_sem.at[lax.rem(w, 4), i])
                for i, k in enumerate((k_dg, k_du, k_mid))
            ]

        def open_half(w):
            for copy in fetch_w(w):
                copy.wait()

            @pl.when(w + 2 < n)
            def _():
                for copy in fetch_w(w + 2):
                    copy.start()

        def term_of(i, m, slot, j):
            left = (h_ring, h_ring, y_ring)[i]
            r = pl.ds(j * 256, 256)
            return w_term([left[2 * m], left[2 * m + 1]], [win[slot, i, 0, r, :], win[slot, i, 1, r, :]])

        def half_tile(i, j):
            def add(w):
                w_add(acc.at[i * per + (odd(w)) * (per // 2) + j], term_of(i, half_of(w), lax.rem(w, 4), j))

            return add

        half_tiles = [half_tile(i, j) for i in range(3) for j in range(per // 2)]

        @pl.when(rest > 0)
        def _():
            for copy in fetch_st(st, 0, n - rest):
                copy.start()

        @pl.when(w_lag < 2)
        def _():
            for w in range(2):
                for copy in fetch_w(w):
                    copy.start()

        for block in range(acc.shape[0]):
            acc[block] = jnp.zeros(acc.shape[1:], f32)

        def only_b(j, _):
            forward_backward(st, 0, n, None, n - rest + j)

            @pl.when((j > 0) & (w_lag > 1))
            def _():
                for copy in fetch_w(j - 1):
                    copy.start()

            return 0

        lax.fori_loop(0, w_lag, only_b, 0)

        def b_and_w(j, _):
            forward_backward(st, 0, n, None, n - rest + j, None, j - w_lag, open_half, half_tiles)
            return 0

        lax.fori_loop(w_lag, rest, b_and_w, 0)
        for c in (n - 2, n - 1):
            for copy in keep_d(c):
                copy.wait()

        done = rest - w_lag

        @pl.when(odd(done) == 1)
        def _():
            open_half(done)
            for tile in half_tiles:
                tile(done)

        def open_whole(m):
            with jax.named_scope("wait_w"):
                for w in (2 * m, 2 * m + 1):
                    for copy in fetch_w(w):
                        copy.wait()

        def whole_w(m, _):
            open_whole(m)
            for w in (2 * m + 2, 2 * m + 3):
                for copy in fetch_w(w):
                    copy.start()
            with jax.named_scope("WW"):
                for i, j in ((i, j) for i in range(3) for j in range(per)):
                    w_add(acc.at[i * per + j], term_of(i, m, 2 * odd(m) + j // (per // 2), j % (per // 2)))
            return 0

        lax.fori_loop((done + 1) // 2, micro - 1, whole_w, 0)

        m = micro - 1
        open_whole(m)
        outs = []
        for i, o in enumerate((o_gate, o_up, o_down)):
            for j in range(per):
                term = term_of(i, m, 2 * odd(m) + j // (per // 2), j % (per // 2))
                at = i * per + j
                h_ring[at] = (acc[at] + rounded(term)).astype(bf16)
                outs.append(pltpu.make_async_copy(h_ring.at[at], o.at[0, :, pl.ds(j * 256, 256)], io_sem.at[5 + at]))
            for copy in outs[-per:]:
                copy.start()
        with jax.named_scope("out"):
            for copy in outs:
                copy.wait()

    held = pltpu.VMEM((2, ff, CHUNK), f32)
    pl.run_scoped(phase_w, held, held, pltpu.VMEM((3 * per, rows, 256), f32), pltpu.VMEM((4, 3, 2, half, CHUNK), bf16))
    for c in range(n - SENDS, n):

        @pl.when(me < stages - 1)
        def _():
            send_f(c).wait_send()

        @pl.when(me > 0)
        def _():
            send_b(c).wait_send()


def solution(mesh):
    stages = mesh.shape["pp"]

    def step(x, dy, w_gate, w_up, w_down):
        micro, d = x.shape[0], x.shape[2]
        ff = w_gate.shape[2]
        n = 2 * micro
        hbm = pl.BlockSpec(memory_space=pltpu.HBM)
        out = jax.ShapeDtypeStruct((1, d, ff), bf16)
        kept = jax.ShapeDtypeStruct((n, ff, CHUNK), f32)
        paired = jax.ShapeDtypeStruct((micro, 2, ff, CHUNK), bf16)
        dma = pltpu.SemaphoreType.DMA
        d_gate, d_up, d_down, *_ = pl.pallas_call(
            functools.partial(kernel, stages, micro),
            out_shape=[out, out, out, kept, kept, paired, paired, paired],
            in_specs=[hbm] * 5,
            out_specs=[hbm] * 8,
            scratch_shapes=[
                pltpu.VMEM((n, d, CHUNK), bf16),
                pltpu.VMEM((n, d, CHUNK), bf16),
                pltpu.VMEM((2, ff, CHUNK), bf16),
                pltpu.VMEM((2, ff, CHUNK), bf16),
                pltpu.VMEM((SENDS, d, CHUNK), bf16),
                pltpu.VMEM((SENDS, d, CHUNK), bf16),
                pltpu.VMEM((d, ff), bf16),
                pltpu.VMEM((d, ff), bf16),
                pltpu.VMEM((ff, d), bf16),
                dma((n,)),
                dma((n,)),
                dma((SENDS,)),
                dma((SENDS,)),
                dma((3, 2)),
                dma((2, 2)),
                dma((2, 2)),
                dma((4, 3)),
                dma((5 + 3 * ff // 256,)),
            ],
            compiler_params=pltpu.CompilerParams(collective_id=0, has_side_effects=True, vmem_limit_bytes=67043328),
        )(x, dy, w_gate, w_up, w_down)
        return d_gate, d_up, jnp.swapaxes(d_down, 1, 2)

    return jax.shard_map(
        step,
        mesh=mesh,
        in_specs=(P("rep", None, None),) * 2 + (P("pp", None, None),) * 3,
        out_specs=(P(("rep", "pp"), None, None),) * 3,
        check_vma=False,
    )
```

```python
import functools

import jax
import jax.numpy as jnp
from jax import lax
from jax.experimental import pallas as pl
from jax.experimental.pallas import tpu as pltpu
from jax.sharding import PartitionSpec as P

f32, bf16 = jnp.float32, jnp.bfloat16
MESH = pl.DeviceIdType.MESH
CHUNK = 256
SENDS = 5
SUB = 64
LEADS = (32, 25, 20, 17, 12, 9, 4, 1)


def dot(a, b):
    return lax.dot_general(a, b, (((1,), (0,)), ((), ())), preferred_element_type=f32)


def dot_t(a, b):
    return lax.dot_general(a, b, (((1,), (1,)), ((), ())), preferred_element_type=f32)


def rounded(v):
    return v.astype(bf16).astype(f32)


def tiles(total, size):
    return [pl.ds(i, size) for i in range(0, total, size)]


def folded(v):
    while v.shape[0] > 8:
        rows = v.shape[0] // 2
        v = v[:rows] + v[rows:]
    return v


def inverse_rms(h):
    total = None
    for r in tiles(h.shape[0], SUB):
        wide = h[r, :].astype(f32)
        part = folded(wide * wide)
        total = part if total is None else total + part
    return lax.rsqrt(jnp.sum(total, 0, keepdims=True) * (1.0 / h.shape[0]) + 1e-6)


def transpose_into(dst, src, rows, cols):
    for r in tiles(rows, 128):
        for c in tiles(cols, 128):
            dst[c, r] = src[r, c].T


def f_norm(h, a, out):
    scale = inverse_rms(h)
    for r in tiles(h.shape[0], SUB):
        a[r, :] = (h[r, :].astype(f32) * scale).astype(bf16)
        out[r, :] = h[r, :]


def f_up(w_gate, w_up, a, s_out, t_out, mid):
    for r in tiles(mid.shape[0], 256):
        gate = dot(w_gate[r, :], a[...])
        up = dot(w_up[r, :], a[...])
        for i in range(0, 256, SUB):
            g, u, q = gate[i : i + SUB], up[i : i + SUB], pl.ds(r.start + i, SUB)
            sig = 1.0 / (1.0 + jnp.exp(-g))
            s = g * sig
            s_out[q, :] = s
            t_out[q, :] = u * (sig + s * (1.0 - sig))
            mid[q, :] = (s * u).astype(bf16)


def f_down(w_down, mid, out):
    for r in tiles(out.shape[0], 320):
        o = dot(w_down[r, :], mid[...])
        for i in range(0, 320, SUB):
            out[pl.ds(r.start + i, SUB), :] += o[i : i + SUB].astype(bf16)


def b_mid(w_down, dy, s_in, t_in, dg, du):
    for r in tiles(dg.shape[0], 256):
        d = dot(w_down[r, :], dy[...])
        for i in range(0, 256, SUB):
            dm, q = rounded(d[i : i + SUB]), pl.ds(r.start + i, SUB)
            dg[q, :] = (dm * t_in[q, :]).astype(bf16)
            du[q, :] = (dm * s_in[q, :]).astype(bf16)


def b_in(w_gate, w_up, dg, du, h, da):
    total = None
    for r in tiles(da.shape[0], 320):
        by_gate = dot(w_gate[r, :], dg[...])
        by_up = dot(w_up[r, :], du[...])
        for i in range(0, 320, SUB):
            q = pl.ds(r.start + i, SUB)
            d = by_gate[i : i + SUB].astype(bf16) + by_up[i : i + SUB].astype(bf16)
            da[q, :] = d
            part = folded(d.astype(f32) * h[q, :].astype(f32))
            total = part if total is None else total + part
    return jnp.sum(total, 0, keepdims=True)


def b_norm(total, scale, h, dy, out):
    k = scale * scale * scale * total * (1.0 / h.shape[0])
    for q in tiles(h.shape[0], SUB):
        wide = h[q, :].astype(f32)
        dh = out[q, :].astype(f32) * scale - wide * k
        out[q, :] = dy[q, :] + dh.astype(bf16)
        h[q, :] = (wide * scale).astype(bf16)


def w_term(left, right):
    return dot_t(left[0], right[0]) + dot_t(left[1], right[1])


def w_add(acc, term):
    acc[...] += rounded(term)


def odd(i):
    return lax.rem(i, 2)


def half_of(i):
    return lax.div(i, 2)


def kernel(stages, micro, x, dy, w_gate, w_up, w_down, o_gate, o_up, o_down, k_s, k_t, k_mid, k_dg, k_du,
           h_ring, y_ring, dg, du, sends, wg, wu, wd,
           h_sem, y_sem, send_sem, fo_sem, bi_sem, bo_sem, wi_sem, io_sem):
    me = lax.axis_index("pp")
    first, last = me == 0, me == stages - 1
    n = 2 * micro
    hidden = wd.shape[0]
    half = hidden // 2
    lead = sum(jnp.where(me == s, v, 0) for s, v in enumerate(LEADS))
    w_lag = jnp.where(last, 0, jnp.where(lead > n - 5, 4, 1))
    rest = jnp.where(last, 0, lead)

    barrier = pltpu.get_barrier_semaphore()

    @pl.when(me > 0)
    def _():
        pl.semaphore_signal(barrier, inc=1, device_id={"pp": me - 1}, device_id_type=MESH)

    @pl.when(me < stages - 1)
    def _():
        pl.semaphore_signal(barrier, inc=1, device_id={"pp": me + 1}, device_id_type=MESH)

    weights_in = [pltpu.make_async_copy(w.at[0], v, io_sem.at[2 + i]) for i, (w, v) in enumerate(((w_gate, wg), (w_up, wu), (w_down, wd)))]
    for copy in weights_in[:2]:
        copy.start()

    f_places = jnp.where(odd(me) == 1, SENDS - 2, 2)
    b_places = SENDS - f_places

    def f_place(c):
        return lax.rem(c, f_places)

    def b_place(c):
        return f_places + lax.rem(c, b_places)

    def send_f(c):
        place = f_place(c)
        return pltpu.make_async_remote_copy(sends.at[place], h_ring.at[c], send_sem.at[place], h_sem.at[c], device_id={"pp": me + 1}, device_id_type=MESH)

    def send_b(c):
        place = b_place(c)
        return pltpu.make_async_remote_copy(sends.at[place], y_ring.at[c], send_sem.at[place], y_sem.at[c], device_id={"pp": me - 1}, device_id_type=MESH)

    def keep_st(st, c):
        return [pltpu.make_async_copy(v.at[odd(c)], k.at[c], fo_sem.at[i, odd(c)]) for i, (v, k) in enumerate(zip(st, (k_s, k_t)))]

    def fetch_st(st, hold, c):
        return [pltpu.make_async_copy(k.at[c], v.at[hold + odd(c)], bi_sem.at[i, odd(c)]) for i, (v, k) in enumerate(zip(st, (k_s, k_t)))]

    def keep_d(c):
        return [pltpu.make_async_copy(v.at[odd(c)], k.at[half_of(c), odd(c)], bo_sem.at[i, odd(c)]) for i, (v, k) in enumerate(((dg, k_dg), (du, k_du)))]

    def forward_backward(st, hold, until, cf, cb, fwd_refs=None, w=None, w_open=None, w_tiles=None):
        if cf is not None:
            wgt, wut, wdt, mid, a_now = fwd_refs

            def keep_mid(c):
                return pltpu.make_async_copy(mid.at[odd(c)], k_mid.at[half_of(c), odd(c)], fo_sem.at[2, odd(c)])

            @pl.when(me > 0)
            def _():
                with jax.named_scope("wait_h"):
                    send_f(cf).wait_recv()

            @pl.when(cf >= 2)
            def _():
                keep_mid(cf - 2).wait()

            @pl.when((cf >= 2) & (me < stages - 1))
            def _():
                for copy in keep_st(st, cf - 2):
                    copy.wait()

            @pl.when((cf >= f_places) & (me < stages - 1))
            def _():
                with jax.named_scope("wait_fs"):
                    send_f(cf - f_places).wait_send()

        if cb is not None:

            @pl.when(me < stages - 1)
            def _():
                with jax.named_scope("wait_y"):
                    send_b(cb).wait_recv()
                with jax.named_scope("wait_st"):
                    for copy in fetch_st(st, hold, cb):
                        copy.wait()

                @pl.when(cb + 1 < until)
                def _():
                    for copy in fetch_st(st, hold, cb + 1):
                        copy.start()

            @pl.when(cb >= 2)
            def _():
                with jax.named_scope("wait_d"):
                    for copy in keep_d(cb - 2):
                        copy.wait()

            @pl.when((cb >= b_places) & (me > 0))
            def _():
                with jax.named_scope("wait_bs"):
                    send_b(cb - b_places).wait_send()

        if w is not None:
            with jax.named_scope("wait_w"):
                w_open(w)
        with jax.named_scope(("F" if cf is not None else "") + ("B" if cb is not None else "") + ("W" if w is not None else "")):
            if cb is not None:
                slot, out = hold + odd(cb), sends.at[b_place(cb)]
                b_mid(wd, y_ring.at[cb], st[0].at[slot], st[1].at[slot], dg.at[odd(cb)], du.at[odd(cb)])
                scale = inverse_rms(h_ring.at[cb])
            if w is not None:
                for tile in w_tiles[: len(w_tiles) // 2]:
                    tile(w)
            if cf is not None:
                f_norm(h_ring.at[cf], a_now, sends.at[f_place(cf)])
                f_up(wgt, wut, a_now, st[0].at[odd(cf)], st[1].at[odd(cf)], mid.at[odd(cf)])
            if cb is not None:
                total = b_in(wg, wu, dg.at[odd(cb)], du.at[odd(cb)], h_ring.at[cb], out)
            if w is not None:
                for tile in w_tiles[len(w_tiles) // 2 :]:
                    tile(w)
            if cb is not None:
                b_norm(total, scale, h_ring.at[cb], y_ring.at[cb], out)
            if cf is not None:
                f_down(wdt, mid.at[odd(cf)], sends.at[f_place(cf)])

        if cb is not None:

            @pl.when(me > 0)
            def _():
                send_b(cb).start()

        if cf is not None:

            @pl.when(me < stages - 1)
            def _():
                send_f(cf).start()
                for copy in keep_st(st, cf):
                    copy.start()

            keep_mid(cf).start()
        if cb is not None:
            for copy in keep_d(cb):
                copy.start()

    def phase_f(st_s, st_t, wgt, wut, wdt, mid, a_now, stage_in):
        def load(src, c, slot):
            return pltpu.make_async_copy(src.at[half_of(c), pl.ds(odd(c) * CHUNK, CHUNK), :], stage_in.at[slot], io_sem.at[slot])

        def take_x(c):
            @pl.when(first & (c < n))
            def _():
                load(x, c, odd(c)).wait()
                transpose_into(h_ring.at[c], stage_in.at[odd(c)], CHUNK, wd.shape[1])

                @pl.when(c + 2 < n)
                def _():
                    load(x, c + 2, odd(c)).start()

        @pl.when(first)
        def _():
            load(x, 0, 0).start()
            load(x, 1, 1).start()

        @pl.when(last)
        def _():
            load(dy, 0, 0).start()
            load(dy, 1, 1).start()

        refs = (wgt, wut, wdt, mid, a_now)
        st = (st_s, st_t)
        hold = jnp.where(last, 0, 2)

        for i, (turned, w) in enumerate(((wgt, wg), (wut, wu), (wdt, wd))):
            weights_in[i].wait()
            if i == 0:
                weights_in[2].start()
            transpose_into(turned, w, *w.shape)
        take_x(0)
        pl.semaphore_wait(barrier, jnp.where(first | last, 1, 2))

        @pl.when(last)
        def _():
            def one(c, _):
                load(dy, c, odd(c)).wait()
                transpose_into(y_ring.at[c], stage_in.at[odd(c)], CHUNK, wd.shape[1])

                @pl.when(c + 2 < n)
                def _():
                    load(dy, c + 2, odd(c)).start()

                return 0

            lax.fori_loop(0, n, one, 0)

        def only_f(c, _):
            forward_backward(st, hold, n, c, None, refs)

            @pl.when((c == 2) & (lead < n) & (me < stages - 1))
            def _():
                for copy in fetch_st(st, hold, 0):
                    copy.start()

            take_x(c + 1)
            return 0

        lax.fori_loop(0, lead, only_f, 0)

        def both(c, _):
            forward_backward(st, hold, n - lead, lead + c, c, refs)
            take_x(lead + c + 1)
            return 0

        lax.fori_loop(0, n - lead, both, 0)

        def only_b(c, _):
            forward_backward(st, hold, n, None, c)
            return 0

        lax.fori_loop(n - lead, n - rest, only_b, 0)
        for c in (n - 2, n - 1):
            pltpu.make_async_copy(mid.at[odd(c)], k_mid.at[half_of(c), odd(c)], fo_sem.at[2, odd(c)]).wait()

            @pl.when(me < stages - 1)
            def _():
                for copy in keep_st(st, c):
                    copy.wait()

    rows, ff = w_gate.shape[1:]
    shapes = (ff, rows), (ff, rows), (rows, ff), (2, ff, CHUNK), (rows, CHUNK), (2, CHUNK, rows)
    wide = pltpu.VMEM((4, ff, CHUNK), f32)
    pl.run_scoped(phase_f, wide, wide, *(pltpu.VMEM(shape, bf16) for shape in shapes))
    per = hidden // 256

    def phase_w(st_s, st_t, acc, win):
        st = (st_s, st_t)

        def fetch_w(w):
            return [
                pltpu.make_async_copy(k.at[half_of(w), :, pl.ds((odd(w)) * half, half), :], win.at[lax.rem(w, 4), i], wi_sem.at[lax.rem(w, 4), i])
                for i, k in enumerate((k_dg, k_du, k_mid))
            ]

        def open_half(w):
            for copy in fetch_w(w):
                copy.wait()

            for copy in fetch_w(w + 1):
                copy.start()

        def term_of(i, m, slot, j):
            left = (h_ring, h_ring, y_ring)[i]
            r = pl.ds(j * 256, 256)
            return w_term([left[2 * m], left[2 * m + 1]], [win[slot, i, 0, r, :], win[slot, i, 1, r, :]])

        def half_tile(i, j):
            def add(w):
                w_add(acc.at[i * per + (odd(w)) * (per // 2) + j], term_of(i, half_of(w), lax.rem(w, 4), j))

            return add

        half_tiles = [half_tile(i, j) for i in range(3) for j in range(per // 2)]

        @pl.when(rest > 0)
        def _():
            for copy in fetch_st(st, 0, n - rest):
                copy.start()

        @pl.when(w_lag < 2)
        def _():
            for copy in fetch_w(0):
                copy.start()

        @pl.when(last)
        def _():
            for copy in fetch_w(1):
                copy.start()

        for block in range(acc.shape[0]):
            acc[block] = jnp.zeros(acc.shape[1:], f32)

        def only_b(j, _):
            forward_backward(st, 0, n, None, n - rest + j)

            @pl.when((w_lag > 1) & (j == w_lag - 1))
            def _():
                for copy in fetch_w(0):
                    copy.start()

            return 0

        lax.fori_loop(0, w_lag, only_b, 0)

        def b_and_w(j, _):
            forward_backward(st, 0, n, None, n - rest + j, None, j - w_lag, open_half, half_tiles)
            return 0

        lax.fori_loop(w_lag, rest, b_and_w, 0)
        for c in (n - 2, n - 1):
            for copy in keep_d(c):
                copy.wait()

        done = rest - w_lag

        @pl.when(odd(done) == 1)
        def _():
            open_half(done)
            for tile in half_tiles:
                tile(done)

        @pl.when(jnp.logical_not(last))
        def _():
            for copy in fetch_w(2 * half_of(done + 1) + 1):
                copy.start()

        def open_whole(m):
            with jax.named_scope("wait_w"):
                for w in (2 * m, 2 * m + 1):
                    for copy in fetch_w(w):
                        copy.wait()

        def whole_w(m, _):
            open_whole(m)
            for w in (2 * m + 2, 2 * m + 3):
                for copy in fetch_w(w):
                    copy.start()
            with jax.named_scope("WW"):
                for i, j in ((i, j) for i in range(3) for j in range(per)):
                    w_add(acc.at[i * per + j], term_of(i, m, 2 * odd(m) + j // (per // 2), j % (per // 2)))
            return 0

        lax.fori_loop(half_of(done + 1), micro - 1, whole_w, 0)

        m = micro - 1
        open_whole(m)

        def finish(i, take):
            for j in range(per):
                take(j, (acc[i * per + j] + rounded(term_of(i, m, 2 * odd(m) + j // (per // 2), j % (per // 2)))).astype(bf16))

        def take_down(j, v):
            h_ring[j] = v

        def take_gate(j, v):
            o_gate[0, :, j * 256 : (j + 1) * 256] = v

        def take_up(j, v):
            o_up[0, :, j * 256 : (j + 1) * 256] = v

        finish(2, take_down)
        finish(0, take_gate)
        for j in range(per):
            transpose_into(o_down.at[0, pl.ds(j * 256, 256), :], h_ring.at[j], rows, 256)
        finish(1, take_up)

    held = pltpu.VMEM((2, ff, CHUNK), f32)
    pl.run_scoped(phase_w, held, held, pltpu.VMEM((3 * per, rows, 256), f32), pltpu.VMEM((4, 3, 2, half, CHUNK), bf16))

    @pl.when(me < stages - 1)
    def _():
        def sent(c, _):
            send_f(c).wait_send()
            return 0

        lax.fori_loop(n - f_places, n, sent, 0)

    @pl.when(me > 0)
    def _():
        def sent(c, _):
            send_b(c).wait_send()
            return 0

        lax.fori_loop(n - b_places, n, sent, 0)


def solution(mesh):
    stages = mesh.shape["pp"]

    def step(x, dy, w_gate, w_up, w_down):
        micro, d = x.shape[0], x.shape[2]
        ff = w_gate.shape[2]
        n = 2 * micro
        hbm = pl.BlockSpec(memory_space=pltpu.HBM)
        out = pltpu.VMEM((1, d, ff), bf16)
        kept = jax.ShapeDtypeStruct((n, ff, CHUNK), f32)
        paired = jax.ShapeDtypeStruct((micro, 2, ff, CHUNK), bf16)
        dma = pltpu.SemaphoreType.DMA
        d_gate, d_up, d_down, *_ = pl.pallas_call(
            functools.partial(kernel, stages, micro),
            out_shape=[out, out, pltpu.VMEM((1, ff, d), bf16), kept, kept, paired, paired, paired],
            in_specs=[hbm] * 5,
            out_specs=[pl.BlockSpec(memory_space=pltpu.VMEM)] * 3 + [hbm] * 5,
            scratch_shapes=[
                pltpu.VMEM((n, d, CHUNK), bf16),
                pltpu.VMEM((n, d, CHUNK), bf16),
                pltpu.VMEM((2, ff, CHUNK), bf16),
                pltpu.VMEM((2, ff, CHUNK), bf16),
                pltpu.VMEM((SENDS, d, CHUNK), bf16),
                pltpu.VMEM((d, ff), bf16),
                pltpu.VMEM((d, ff), bf16),
                pltpu.VMEM((ff, d), bf16),
                dma((n,)),
                dma((n,)),
                dma((SENDS,)),
                dma((3, 2)),
                dma((2, 2)),
                dma((2, 2)),
                dma((4, 3)),
                dma((5,)),
            ],
            compiler_params=pltpu.CompilerParams(collective_id=0, has_side_effects=True, vmem_limit_bytes=61100000),
        )(x, dy, w_gate, w_up, w_down)
        return d_gate, d_up, d_down

    return jax.shard_map(
        step,
        mesh=mesh,
        in_specs=(P("rep", None, None),) * 2 + (P("pp", None, None),) * 3,
        out_specs=(P(("rep", "pp"), None, None),) * 3,
        check_vma=False,
    )
```

```python
import functools

import jax
import jax.numpy as jnp
from jax import lax
from jax.experimental import pallas as pl
from jax.experimental.pallas import tpu as pltpu
from jax.sharding import PartitionSpec as P

f32, bf16 = jnp.float32, jnp.bfloat16
MESH = pl.DeviceIdType.MESH
CHUNK = 256
SENDS = 5
SUB = 64
LEADS = (32, 25, 20, 17, 12, 9, 4, 1)


def dot(a, b):
    return lax.dot_general(a, b, (((1,), (0,)), ((), ())), preferred_element_type=f32)


def dot_t(a, b):
    return lax.dot_general(a, b, (((1,), (1,)), ((), ())), preferred_element_type=f32)


def rounded(v):
    return v.astype(bf16).astype(f32)


def tiles(total, size):
    return [pl.ds(i, size) for i in range(0, total, size)]


def folded(v):
    while v.shape[0] > 8:
        rows = v.shape[0] // 2
        v = v[:rows] + v[rows:]
    return v


def inverse_rms(h):
    total = None
    for r in tiles(h.shape[0], SUB):
        wide = h[r, :].astype(f32)
        part = folded(wide * wide)
        total = part if total is None else total + part
    return lax.rsqrt(jnp.sum(total, 0, keepdims=True) * (1.0 / h.shape[0]) + 1e-6)


def transpose_into(dst, src, rows, cols):
    for r in tiles(rows, 128):
        for c in tiles(cols, 128):
            dst[c, r] = src[r, c].T


def f_norm(h, a, out):
    scale = inverse_rms(h)
    for r in tiles(h.shape[0], SUB):
        a[r, :] = (h[r, :].astype(f32) * scale).astype(bf16)
        out[r, :] = h[r, :]


def f_up(w_gate, w_up, a, s_out, t_out, mid):
    for r in tiles(mid.shape[0], 256):
        gate = dot(w_gate[r, :], a[...])
        up = dot(w_up[r, :], a[...])
        for i in range(0, 256, SUB):
            g, u, q = gate[i : i + SUB], up[i : i + SUB], pl.ds(r.start + i, SUB)
            sig = 1.0 / (1.0 + jnp.exp(-g))
            s = g * sig
            s_out[q, :] = s
            t_out[q, :] = u * (sig + s * (1.0 - sig))
            mid[q, :] = (s * u).astype(bf16)


def f_down(w_down, mid, out):
    for r in tiles(out.shape[0], 320):
        o = dot(w_down[r, :], mid[...])
        for i in range(0, 320, SUB):
            out[pl.ds(r.start + i, SUB), :] += o[i : i + SUB].astype(bf16)


def b_mid(w_down, dy, s_in, t_in, dg, du):
    for r in tiles(dg.shape[0], 256):
        d = dot(w_down[r, :], dy[...])
        for i in range(0, 256, SUB):
            dm, q = rounded(d[i : i + SUB]), pl.ds(r.start + i, SUB)
            dg[q, :] = (dm * t_in[q, :]).astype(bf16)
            du[q, :] = (dm * s_in[q, :]).astype(bf16)


def b_in(w_gate, w_up, dg, du, h, da):
    total = None
    for r in tiles(da.shape[0], 320):
        by_gate = dot(w_gate[r, :], dg[...])
        by_up = dot(w_up[r, :], du[...])
        for i in range(0, 320, SUB):
            q = pl.ds(r.start + i, SUB)
            d = by_gate[i : i + SUB].astype(bf16) + by_up[i : i + SUB].astype(bf16)
            da[q, :] = d
            part = folded(d.astype(f32) * h[q, :].astype(f32))
            total = part if total is None else total + part
    return jnp.sum(total, 0, keepdims=True)


def b_norm(total, scale, h, dy, out):
    k = scale * scale * scale * total * (1.0 / h.shape[0])
    for q in tiles(h.shape[0], SUB):
        wide = h[q, :].astype(f32)
        dh = out[q, :].astype(f32) * scale - wide * k
        out[q, :] = dy[q, :] + dh.astype(bf16)
        h[q, :] = (wide * scale).astype(bf16)


def w_term(left, right):
    return dot_t(left[0], right[0]) + dot_t(left[1], right[1])


def w_add(acc, term):
    acc[...] += rounded(term)


def odd(i):
    return lax.rem(i, 2)


def half_of(i):
    return lax.div(i, 2)


def kernel(stages, micro, x, dy, w_gate, w_up, w_down, o_gate, o_up, o_down, k_s, k_t, k_mid, k_dg, k_du,
           h_ring, y_ring, dg, du, sends, wg, wu, wd,
           h_sem, y_sem, send_sem, fo_sem, bi_sem, bo_sem, wi_sem, io_sem):
    me = lax.axis_index("pp")
    first, last = me == 0, me == stages - 1
    n = 2 * micro
    hidden = wd.shape[0]
    half = hidden // 2
    lead = sum(jnp.where(me == s, v, 0) for s, v in enumerate(LEADS))
    rest = lead - 1
    w_lag = jnp.where(last, 0, jnp.where(rest > n - 5, 3, 1))

    barrier = pltpu.get_barrier_semaphore()

    @pl.when(me > 0)
    def _():
        pl.semaphore_signal(barrier, inc=1, device_id={"pp": me - 1}, device_id_type=MESH)

    @pl.when(me < stages - 1)
    def _():
        pl.semaphore_signal(barrier, inc=1, device_id={"pp": me + 1}, device_id_type=MESH)

    weights_in = [pltpu.make_async_copy(w.at[0], v, io_sem.at[2 + i]) for i, (w, v) in enumerate(((w_gate, wg), (w_up, wu), (w_down, wd)))]
    for copy in weights_in:
        copy.start()

    f_places = jnp.where(odd(me) == 1, SENDS - 2, 2)
    b_places = SENDS - f_places

    def f_place(c):
        return lax.rem(c, f_places)

    def b_place(c):
        return f_places + lax.rem(c, b_places)

    def send_f(c):
        place = f_place(c)
        return pltpu.make_async_remote_copy(sends.at[place], h_ring.at[c], send_sem.at[place], h_sem.at[c], device_id={"pp": me + 1}, device_id_type=MESH)

    def send_b(c):
        place = b_place(c)
        return pltpu.make_async_remote_copy(sends.at[place], y_ring.at[c], send_sem.at[place], y_sem.at[c], device_id={"pp": me - 1}, device_id_type=MESH)

    def keep_st(st, c):
        return [pltpu.make_async_copy(v.at[odd(c)], k.at[c], fo_sem.at[i, odd(c)]) for i, (v, k) in enumerate(zip(st, (k_s, k_t)))]

    def fetch_st(st, hold, c):
        return [pltpu.make_async_copy(k.at[c], v.at[hold + odd(c)], bi_sem.at[i, odd(c)]) for i, (v, k) in enumerate(zip(st, (k_s, k_t)))]

    def keep_d(c):
        return [pltpu.make_async_copy(v.at[odd(c)], k.at[half_of(c), odd(c)], bo_sem.at[i, odd(c)]) for i, (v, k) in enumerate(((dg, k_dg), (du, k_du)))]

    def forward_backward(st, hold, until, cf, cb, fwd_refs=None, w=None, w_open=None, w_tiles=None):
        if cf is not None:
            wgt, wut, wdt, mid, a_now = fwd_refs

            def keep_mid(c):
                return pltpu.make_async_copy(mid.at[odd(c)], k_mid.at[half_of(c), odd(c)], fo_sem.at[2, odd(c)])

            @pl.when(me > 0)
            def _():
                with jax.named_scope("wait_h"):
                    send_f(cf).wait_recv()

            @pl.when(cf >= 2)
            def _():
                keep_mid(cf - 2).wait()

            @pl.when((cf >= 2) & (me < stages - 1))
            def _():
                for copy in keep_st(st, cf - 2):
                    copy.wait()

            @pl.when((cf >= f_places) & (me < stages - 1))
            def _():
                with jax.named_scope("wait_fs"):
                    send_f(cf - f_places).wait_send()

        if cb is not None:

            @pl.when(me < stages - 1)
            def _():
                with jax.named_scope("wait_y"):
                    send_b(cb).wait_recv()
                with jax.named_scope("wait_st"):
                    for copy in fetch_st(st, hold, cb):
                        copy.wait()

                @pl.when(cb + 1 < until)
                def _():
                    for copy in fetch_st(st, hold, cb + 1):
                        copy.start()

            @pl.when(cb >= 2)
            def _():
                with jax.named_scope("wait_d"):
                    for copy in keep_d(cb - 2):
                        copy.wait()

            @pl.when((cb >= b_places) & (me > 0))
            def _():
                with jax.named_scope("wait_bs"):
                    send_b(cb - b_places).wait_send()

        if w is not None:
            with jax.named_scope("wait_w"):
                w_open(w)
        with jax.named_scope(("F" if cf is not None else "") + ("B" if cb is not None else "") + ("W" if w is not None else "")):
            if cb is not None:
                slot, out = hold + odd(cb), sends.at[b_place(cb)]
                b_mid(wd, y_ring.at[cb], st[0].at[slot], st[1].at[slot], dg.at[odd(cb)], du.at[odd(cb)])
                scale = inverse_rms(h_ring.at[cb])
            if w is not None:
                for tile in w_tiles[: len(w_tiles) // 2]:
                    tile(w)
            if cf is not None:
                f_norm(h_ring.at[cf], a_now, sends.at[f_place(cf)])
                f_up(wgt, wut, a_now, st[0].at[odd(cf)], st[1].at[odd(cf)], mid.at[odd(cf)])
            if cb is not None:
                total = b_in(wg, wu, dg.at[odd(cb)], du.at[odd(cb)], h_ring.at[cb], out)
            if w is not None:
                for tile in w_tiles[len(w_tiles) // 2 :]:
                    tile(w)
            if cb is not None:
                b_norm(total, scale, h_ring.at[cb], y_ring.at[cb], out)
            if cf is not None:
                f_down(wdt, mid.at[odd(cf)], sends.at[f_place(cf)])

        if cb is not None:

            @pl.when(me > 0)
            def _():
                send_b(cb).start()

        if cf is not None:

            @pl.when(me < stages - 1)
            def _():
                send_f(cf).start()
                for copy in keep_st(st, cf):
                    copy.start()

            keep_mid(cf).start()
        if cb is not None:
            for copy in keep_d(cb):
                copy.start()

    def phase_f(st_s, st_t, wgt, wut, wdt, mid, a_now, stage_in):
        def load(src, c, slot):
            return pltpu.make_async_copy(src.at[half_of(c), pl.ds(odd(c) * CHUNK, CHUNK), :], stage_in.at[slot], io_sem.at[slot])

        def take_x(c):
            @pl.when(first & (c < n))
            def _():
                load(x, c, odd(c)).wait()
                transpose_into(h_ring.at[c], stage_in.at[odd(c)], CHUNK, wd.shape[1])

                @pl.when(c + 2 < n)
                def _():
                    load(x, c + 2, odd(c)).start()

        @pl.when(first)
        def _():
            load(x, 0, 0).start()
            load(x, 1, 1).start()

        @pl.when(last)
        def _():
            load(dy, 0, 0).start()
            load(dy, 1, 1).start()

        refs = (wgt, wut, wdt, mid, a_now)
        st = (st_s, st_t)
        hold = jnp.where(last, 0, 2)

        for i, (turned, w) in enumerate(((wgt, wg), (wut, wu), (wdt, wd))):
            weights_in[i].wait()
            transpose_into(turned, w, *w.shape)
        take_x(0)
        pl.semaphore_wait(barrier, jnp.where(first | last, 1, 2))

        @pl.when(last)
        def _():
            def one(c, _):
                load(dy, c, odd(c)).wait()
                transpose_into(y_ring.at[c], stage_in.at[odd(c)], CHUNK, wd.shape[1])

                @pl.when(c + 2 < n)
                def _():
                    load(dy, c + 2, odd(c)).start()

                return 0

            lax.fori_loop(0, n, one, 0)

        def only_f(c, _):
            forward_backward(st, hold, n, c, None, refs)

            @pl.when((c == 2) & (me < stages - 1))
            def _():
                for copy in fetch_st(st, hold, 0):
                    copy.start()

            take_x(c + 1)
            return 0

        lax.fori_loop(0, lead, only_f, 0)

        def both(c, _):
            forward_backward(st, hold, n - rest, lead + c, c, refs)
            take_x(lead + c + 1)
            return 0

        lax.fori_loop(0, n - lead, both, 0)

        def only_b(c, _):
            forward_backward(st, hold, n - rest, None, c)
            return 0

        lax.fori_loop(n - lead, n - rest, only_b, 0)
        for c in (n - 2, n - 1):
            pltpu.make_async_copy(mid.at[odd(c)], k_mid.at[half_of(c), odd(c)], fo_sem.at[2, odd(c)]).wait()

            @pl.when(me < stages - 1)
            def _():
                for copy in keep_st(st, c):
                    copy.wait()

    rows, ff = w_gate.shape[1:]
    shapes = (ff, rows), (ff, rows), (rows, ff), (2, ff, CHUNK), (rows, CHUNK), (2, CHUNK, rows)
    wide = pltpu.VMEM((4, ff, CHUNK), f32)
    pl.run_scoped(phase_f, wide, wide, *(pltpu.VMEM(shape, bf16) for shape in shapes))
    per = hidden // 256

    def phase_w(st_s, st_t, acc, win):
        st = (st_s, st_t)

        def fetch_w(w):
            return [
                pltpu.make_async_copy(k.at[half_of(w), :, pl.ds((odd(w)) * half, half), :], win.at[lax.rem(w, 4), i], wi_sem.at[lax.rem(w, 4), i])
                for i, k in enumerate((k_dg, k_du, k_mid))
            ]

        def fetch_pair(w):
            for copy in fetch_w(w) + fetch_w(w + 1):
                copy.start()

        def open_half(w):
            for copy in fetch_w(w):
                copy.wait()

            @pl.when(odd(w) == 1)
            def _():
                fetch_pair(w + 1)

        def term_of(i, m, slot, j):
            left = (h_ring, h_ring, y_ring)[i]
            r = pl.ds(j * 256, 256)
            return w_term([left[2 * m], left[2 * m + 1]], [win[slot, i, 0, r, :], win[slot, i, 1, r, :]])

        def half_tile(i, j):
            def add(w):
                w_add(acc.at[i * per + (odd(w)) * (per // 2) + j], term_of(i, half_of(w), lax.rem(w, 4), j))

            return add

        half_tiles = [half_tile(i, j) for i in range(3) for j in range(per // 2)]

        @pl.when(rest > 0)
        def _():
            for copy in fetch_st(st, 0, n - rest):
                copy.start()

        @pl.when(w_lag < 2)
        def _():
            fetch_pair(0)

        for block in range(acc.shape[0]):
            acc[block] = jnp.zeros(acc.shape[1:], f32)

        def only_b(j, _):
            forward_backward(st, 0, n, None, n - rest + j)

            @pl.when((w_lag > 1) & (j == w_lag - 1))
            def _():
                fetch_pair(0)

            return 0

        lax.fori_loop(0, w_lag, only_b, 0)

        def b_and_w(j, _):
            forward_backward(st, 0, n, None, n - rest + j, None, j - w_lag, open_half, half_tiles)
            return 0

        lax.fori_loop(w_lag, rest, b_and_w, 0)
        for c in (n - 2, n - 1):
            for copy in keep_d(c):
                copy.wait()

        done = rest - w_lag

        @pl.when(odd(done) == 1)
        def _():
            open_half(done)
            for tile in half_tiles:
                tile(done)

        def open_whole(m):
            with jax.named_scope("wait_w"):
                for w in (2 * m, 2 * m + 1):
                    for copy in fetch_w(w):
                        copy.wait()

        def whole_w(m, _):
            open_whole(m)
            fetch_pair(2 * m + 2)
            with jax.named_scope("WW"):
                for i, j in ((i, j) for i in range(3) for j in range(per)):
                    w_add(acc.at[i * per + j], term_of(i, m, 2 * odd(m) + j // (per // 2), j % (per // 2)))
            return 0

        lax.fori_loop(half_of(done + 1), micro - 1, whole_w, 0)

        m = micro - 1
        open_whole(m)

        def finish(i, take):
            for j in range(per):
                take(j, (acc[i * per + j] + rounded(term_of(i, m, 2 * odd(m) + j // (per // 2), j % (per // 2)))).astype(bf16))

        def take_down(j, v):
            h_ring[j] = v

        def take_gate(j, v):
            o_gate[0, :, j * 256 : (j + 1) * 256] = v

        def take_up(j, v):
            o_up[0, :, j * 256 : (j + 1) * 256] = v

        finish(2, take_down)
        finish(0, take_gate)
        for j in range(per):
            transpose_into(o_down.at[0, pl.ds(j * 256, 256), :], h_ring.at[j], rows, 256)
        finish(1, take_up)

    held = pltpu.VMEM((2, ff, CHUNK), f32)
    pl.run_scoped(phase_w, held, held, pltpu.VMEM((3 * per, rows, 256), f32), pltpu.VMEM((4, 3, 2, half, CHUNK), bf16))

    @pl.when(me < stages - 1)
    def _():
        def sent(c, _):
            send_f(c).wait_send()
            return 0

        lax.fori_loop(n - f_places, n, sent, 0)

    @pl.when(me > 0)
    def _():
        def sent(c, _):
            send_b(c).wait_send()
            return 0

        lax.fori_loop(n - b_places, n, sent, 0)


def solution(mesh):
    stages = mesh.shape["pp"]

    def step(x, dy, w_gate, w_up, w_down):
        micro, d = x.shape[0], x.shape[2]
        ff = w_gate.shape[2]
        n = 2 * micro
        hbm = pl.BlockSpec(memory_space=pltpu.HBM)
        out = pltpu.VMEM((1, d, ff), bf16)
        kept = jax.ShapeDtypeStruct((n, ff, CHUNK), f32)
        paired = jax.ShapeDtypeStruct((micro, 2, ff, CHUNK), bf16)
        dma = pltpu.SemaphoreType.DMA
        d_gate, d_up, d_down, *_ = pl.pallas_call(
            functools.partial(kernel, stages, micro),
            out_shape=[out, out, pltpu.VMEM((1, ff, d), bf16), kept, kept, paired, paired, paired],
            in_specs=[hbm] * 5,
            out_specs=[pl.BlockSpec(memory_space=pltpu.VMEM)] * 3 + [hbm] * 5,
            scratch_shapes=[
                pltpu.VMEM((n, d, CHUNK), bf16),
                pltpu.VMEM((n, d, CHUNK), bf16),
                pltpu.VMEM((2, ff, CHUNK), bf16),
                pltpu.VMEM((2, ff, CHUNK), bf16),
                pltpu.VMEM((SENDS, d, CHUNK), bf16),
                pltpu.VMEM((d, ff), bf16),
                pltpu.VMEM((d, ff), bf16),
                pltpu.VMEM((ff, d), bf16),
                dma((n,)),
                dma((n,)),
                dma((SENDS,)),
                dma((3, 2)),
                dma((2, 2)),
                dma((2, 2)),
                dma((4, 3)),
                dma((5,)),
            ],
            compiler_params=pltpu.CompilerParams(collective_id=0, has_side_effects=True, vmem_limit_bytes=61100000),
        )(x, dy, w_gate, w_up, w_down)
        return d_gate, d_up, d_down

    return jax.shard_map(
        step,
        mesh=mesh,
        in_specs=(P("rep", None, None),) * 2 + (P("pp", None, None),) * 3,
        out_specs=(P(("rep", "pp"), None, None),) * 3,
        check_vma=False,
    )
```

```python
import functools

import jax
import jax.numpy as jnp
from jax import lax
from jax.experimental import pallas as pl
from jax.experimental.pallas import tpu as pltpu
from jax.sharding import PartitionSpec as P

f32, bf16 = jnp.float32, jnp.bfloat16
MESH = pl.DeviceIdType.MESH
CHUNK = 256
SENDS = 5
SUB = 64
LEADS = (32, 26, 20, 17, 12, 9, 4, 1)


def dot(a, b):
    return lax.dot_general(a, b, (((1,), (0,)), ((), ())), preferred_element_type=f32)


def dot_t(a, b):
    return lax.dot_general(a, b, (((1,), (1,)), ((), ())), preferred_element_type=f32)


def rounded(v):
    return v.astype(bf16).astype(f32)


def tiles(total, size):
    return [pl.ds(i, size) for i in range(0, total, size)]


def folded(v):
    while v.shape[0] > 8:
        rows = v.shape[0] // 2
        v = v[:rows] + v[rows:]
    return v


def inverse_rms(h):
    total = None
    for r in tiles(h.shape[0], SUB):
        wide = h[r, :].astype(f32)
        part = folded(wide * wide)
        total = part if total is None else total + part
    return lax.rsqrt(jnp.sum(total, 0, keepdims=True) * (1.0 / h.shape[0]) + 1e-6)


def transpose_into(dst, src, rows, cols):
    for r in tiles(rows, 128):
        for c in tiles(cols, 128):
            dst[c, r] = src[r, c].T


def f_norm(h, a, out):
    scale = inverse_rms(h)
    for r in tiles(h.shape[0], SUB):
        a[r, :] = (h[r, :].astype(f32) * scale).astype(bf16)
        out[r, :] = h[r, :]


def f_up(w_gate, w_up, a, s_out, t_out, mid):
    for r in tiles(mid.shape[0], 256):
        gate = dot(w_gate[r, :], a[...])
        up = dot(w_up[r, :], a[...])
        for i in range(0, 256, SUB):
            g, u, q = gate[i : i + SUB], up[i : i + SUB], pl.ds(r.start + i, SUB)
            sig = 1.0 / (1.0 + jnp.exp(-g))
            s = g * sig
            s_out[q, :] = s
            t_out[q, :] = u * (sig + s * (1.0 - sig))
            mid[q, :] = (s * u).astype(bf16)


def f_down(w_down, mid, out):
    for r in tiles(out.shape[0], 320):
        o = dot(w_down[r, :], mid[...])
        for i in range(0, 320, SUB):
            out[pl.ds(r.start + i, SUB), :] += o[i : i + SUB].astype(bf16)


def b_mid(w_down, dy, s_in, t_in, dg, du):
    for r in tiles(dg.shape[0], 256):
        d = dot(w_down[r, :], dy[...])
        for i in range(0, 256, SUB):
            dm, q = rounded(d[i : i + SUB]), pl.ds(r.start + i, SUB)
            dg[q, :] = (dm * t_in[q, :]).astype(bf16)
            du[q, :] = (dm * s_in[q, :]).astype(bf16)


def b_in(w_gate, w_up, dg, du, h, da):
    total = None
    for r in tiles(da.shape[0], 320):
        by_gate = dot(w_gate[r, :], dg[...])
        by_up = dot(w_up[r, :], du[...])
        for i in range(0, 320, SUB):
            q = pl.ds(r.start + i, SUB)
            d = by_gate[i : i + SUB].astype(bf16) + by_up[i : i + SUB].astype(bf16)
            da[q, :] = d
            part = folded(d.astype(f32) * h[q, :].astype(f32))
            total = part if total is None else total + part
    return jnp.sum(total, 0, keepdims=True)


def b_norm(total, scale, h, dy, out):
    k = scale * scale * scale * total * (1.0 / h.shape[0])
    for q in tiles(h.shape[0], SUB):
        wide = h[q, :].astype(f32)
        dh = out[q, :].astype(f32) * scale - wide * k
        out[q, :] = dy[q, :] + dh.astype(bf16)
        h[q, :] = (wide * scale).astype(bf16)


def w_term(left, right):
    return dot_t(left[0], right[0]) + dot_t(left[1], right[1])


def w_add(acc, term):
    acc[...] += rounded(term)


def odd(i):
    return lax.rem(i, 2)


def half_of(i):
    return lax.div(i, 2)


def kernel(stages, micro, x, dy, w_gate, w_up, w_down, o_gate, o_up, o_down, k_s, k_t, k_mid, k_dg, k_du,
           h_ring, y_ring, dg, du, sends, wg, wu, wd,
           h_sem, y_sem, send_sem, fo_sem, bi_sem, bo_sem, wi_sem, io_sem):
    me = lax.axis_index("pp")
    first, last = me == 0, me == stages - 1
    n = 2 * micro
    hidden = wd.shape[0]
    half = hidden // 2
    lead = sum(jnp.where(me == s, v, 0) for s, v in enumerate(LEADS))
    rest = lead - 1
    w_lag = jnp.where(last, 0, jnp.where(rest > n - 5, 3, 1))

    barrier = pltpu.get_barrier_semaphore()

    @pl.when(me > 0)
    def _():
        pl.semaphore_signal(barrier, inc=1, device_id={"pp": me - 1}, device_id_type=MESH)

    @pl.when(me < stages - 1)
    def _():
        pl.semaphore_signal(barrier, inc=1, device_id={"pp": me + 1}, device_id_type=MESH)

    weights_in = [pltpu.make_async_copy(w.at[0], v, io_sem.at[2 + i]) for i, (w, v) in enumerate(((w_gate, wg), (w_up, wu), (w_down, wd)))]
    for copy in weights_in:
        copy.start()

    f_places = jnp.where(odd(me) == 1, SENDS - 2, 2)
    b_places = SENDS - f_places

    def f_place(c):
        return lax.rem(c, f_places)

    def b_place(c):
        return f_places + lax.rem(c, b_places)

    def send_f(c):
        place = f_place(c)
        return pltpu.make_async_remote_copy(sends.at[place], h_ring.at[c], send_sem.at[place], h_sem.at[c], device_id={"pp": me + 1}, device_id_type=MESH)

    def send_b(c):
        place = b_place(c)
        return pltpu.make_async_remote_copy(sends.at[place], y_ring.at[c], send_sem.at[place], y_sem.at[c], device_id={"pp": me - 1}, device_id_type=MESH)

    def keep_st(st, c):
        return [pltpu.make_async_copy(v.at[odd(c)], k.at[c], fo_sem.at[i, odd(c)]) for i, (v, k) in enumerate(zip(st, (k_s, k_t)))]

    def fetch_st(st, hold, c):
        return [pltpu.make_async_copy(k.at[c], v.at[hold + odd(c)], bi_sem.at[i, odd(c)]) for i, (v, k) in enumerate(zip(st, (k_s, k_t)))]

    def keep_d(c):
        return [pltpu.make_async_copy(v.at[odd(c)], k.at[half_of(c), odd(c)], bo_sem.at[i, odd(c)]) for i, (v, k) in enumerate(((dg, k_dg), (du, k_du)))]

    def forward_backward(st, hold, until, cf, cb, fwd_refs=None, w=None, w_open=None, w_tiles=None):
        if cf is not None:
            wgt, wut, wdt, mid, a_now = fwd_refs

            def keep_mid(c):
                return pltpu.make_async_copy(mid.at[odd(c)], k_mid.at[half_of(c), odd(c)], fo_sem.at[2, odd(c)])

            @pl.when(me > 0)
            def _():
                with jax.named_scope("wait_h"):
                    send_f(cf).wait_recv()

            @pl.when(cf >= 2)
            def _():
                keep_mid(cf - 2).wait()

            @pl.when((cf >= 2) & (me < stages - 1))
            def _():
                for copy in keep_st(st, cf - 2):
                    copy.wait()

            @pl.when((cf >= f_places) & (me < stages - 1))
            def _():
                with jax.named_scope("wait_fs"):
                    send_f(cf - f_places).wait_send()

        if cb is not None:

            @pl.when(me < stages - 1)
            def _():
                with jax.named_scope("wait_y"):
                    send_b(cb).wait_recv()
                with jax.named_scope("wait_st"):
                    for copy in fetch_st(st, hold, cb):
                        copy.wait()

                @pl.when(cb + 1 < until)
                def _():
                    for copy in fetch_st(st, hold, cb + 1):
                        copy.start()

            @pl.when(cb >= 2)
            def _():
                with jax.named_scope("wait_d"):
                    for copy in keep_d(cb - 2):
                        copy.wait()

            @pl.when((cb >= b_places) & (me > 0))
            def _():
                with jax.named_scope("wait_bs"):
                    send_b(cb - b_places).wait_send()

        if w is not None:
            with jax.named_scope("wait_w"):
                w_open(w)
        with jax.named_scope(("F" if cf is not None else "") + ("B" if cb is not None else "") + ("W" if w is not None else "")):
            if cb is not None:
                slot, out = hold + odd(cb), sends.at[b_place(cb)]
                b_mid(wd, y_ring.at[cb], st[0].at[slot], st[1].at[slot], dg.at[odd(cb)], du.at[odd(cb)])
                scale = inverse_rms(h_ring.at[cb])
            if w is not None:
                for tile in w_tiles[: len(w_tiles) // 2]:
                    tile(w)
            if cf is not None:
                f_norm(h_ring.at[cf], a_now, sends.at[f_place(cf)])
                f_up(wgt, wut, a_now, st[0].at[odd(cf)], st[1].at[odd(cf)], mid.at[odd(cf)])
            if cb is not None:
                total = b_in(wg, wu, dg.at[odd(cb)], du.at[odd(cb)], h_ring.at[cb], out)
            if w is not None:
                for tile in w_tiles[len(w_tiles) // 2 :]:
                    tile(w)
            if cb is not None:
                b_norm(total, scale, h_ring.at[cb], y_ring.at[cb], out)
            if cf is not None:
                f_down(wdt, mid.at[odd(cf)], sends.at[f_place(cf)])

        if cb is not None:

            @pl.when(me > 0)
            def _():
                send_b(cb).start()

        if cf is not None:

            @pl.when(me < stages - 1)
            def _():
                send_f(cf).start()
                for copy in keep_st(st, cf):
                    copy.start()

            keep_mid(cf).start()
        if cb is not None:
            for copy in keep_d(cb):
                copy.start()

    def phase_f(st_s, st_t, wgt, wut, wdt, mid, a_now, stage_in):
        def load(src, c, slot):
            return pltpu.make_async_copy(src.at[half_of(c), pl.ds(odd(c) * CHUNK, CHUNK), :], stage_in.at[slot], io_sem.at[slot])

        def take_x(c):
            @pl.when(first & (c < n))
            def _():
                load(x, c, odd(c)).wait()
                transpose_into(h_ring.at[c], stage_in.at[odd(c)], CHUNK, wd.shape[1])

                @pl.when(c + 2 < n)
                def _():
                    load(x, c + 2, odd(c)).start()

        @pl.when(first)
        def _():
            load(x, 0, 0).start()
            load(x, 1, 1).start()

        @pl.when(last)
        def _():
            load(dy, 0, 0).start()
            load(dy, 1, 1).start()

        refs = (wgt, wut, wdt, mid, a_now)
        st = (st_s, st_t)
        hold = jnp.where(last, 0, 2)

        for i, (turned, w) in enumerate(((wgt, wg), (wut, wu), (wdt, wd))):
            weights_in[i].wait()
            transpose_into(turned, w, *w.shape)
        take_x(0)
        pl.semaphore_wait(barrier, jnp.where(first | last, 1, 2))

        @pl.when(last)
        def _():
            def one(c, _):
                load(dy, c, odd(c)).wait()
                transpose_into(y_ring.at[c], stage_in.at[odd(c)], CHUNK, wd.shape[1])

                @pl.when(c + 2 < n)
                def _():
                    load(dy, c + 2, odd(c)).start()

                return 0

            lax.fori_loop(0, n, one, 0)

        def only_f(c, _):
            forward_backward(st, hold, n, c, None, refs)

            @pl.when((c == 2) & (me < stages - 1))
            def _():
                for copy in fetch_st(st, hold, 0):
                    copy.start()

            take_x(c + 1)
            return 0

        lax.fori_loop(0, lead, only_f, 0)

        def both(c, _):
            forward_backward(st, hold, n - rest, lead + c, c, refs)
            take_x(lead + c + 1)
            return 0

        lax.fori_loop(0, n - lead, both, 0)

        def only_b(c, _):
            forward_backward(st, hold, n - rest, None, c)
            return 0

        lax.fori_loop(n - lead, n - rest, only_b, 0)
        for c in (n - 2, n - 1):
            pltpu.make_async_copy(mid.at[odd(c)], k_mid.at[half_of(c), odd(c)], fo_sem.at[2, odd(c)]).wait()

            @pl.when(me < stages - 1)
            def _():
                for copy in keep_st(st, c):
                    copy.wait()

    rows, ff = w_gate.shape[1:]
    shapes = (ff, rows), (ff, rows), (rows, ff), (2, ff, CHUNK), (rows, CHUNK), (2, CHUNK, rows)
    wide = pltpu.VMEM((4, ff, CHUNK), f32)
    pl.run_scoped(phase_f, wide, wide, *(pltpu.VMEM(shape, bf16) for shape in shapes))
    per = hidden // 256

    def phase_w(st_s, st_t, acc, win):
        st = (st_s, st_t)

        def fetch_w(w):
            return [
                pltpu.make_async_copy(k.at[half_of(w), :, pl.ds((odd(w)) * half, half), :], win.at[lax.rem(w, 4), i], wi_sem.at[lax.rem(w, 4), i])
                for i, k in enumerate((k_dg, k_du, k_mid))
            ]

        done = rest - w_lag

        def fetch_pair(w):
            for copy in fetch_w(w) + fetch_w(w + 1):
                copy.start()

        def open_half(w):
            for copy in fetch_w(w):
                copy.wait()

            @pl.when(w < done)
            def _():
                for copy in fetch_w(w + 1):
                    copy.start()

            @pl.when(w >= done - 1)
            def _():
                for copy in fetch_w(w + 2):
                    copy.start()

        def term_of(i, m, slot, j):
            left = (h_ring, h_ring, y_ring)[i]
            r = pl.ds(j * 256, 256)
            return w_term([left[2 * m], left[2 * m + 1]], [win[slot, i, 0, r, :], win[slot, i, 1, r, :]])

        def half_tile(i, j):
            def add(w):
                w_add(acc.at[i * per + (odd(w)) * (per // 2) + j], term_of(i, half_of(w), lax.rem(w, 4), j))

            return add

        half_tiles = [half_tile(i, j) for i in range(3) for j in range(per // 2)]

        @pl.when(rest > 0)
        def _():
            for copy in fetch_st(st, 0, n - rest):
                copy.start()

        @pl.when(w_lag < 2)
        def _():
            for copy in fetch_w(0):
                copy.start()

        @pl.when(last)
        def _():
            for copy in fetch_w(1):
                copy.start()

        for block in range(acc.shape[0]):
            acc[block] = jnp.zeros(acc.shape[1:], f32)

        def only_b(j, _):
            forward_backward(st, 0, n, None, n - rest + j)

            @pl.when((w_lag > 1) & (j == w_lag - 1))
            def _():
                for copy in fetch_w(0):
                    copy.start()

            return 0

        lax.fori_loop(0, w_lag, only_b, 0)

        def b_and_w(j, _):
            forward_backward(st, 0, n, None, n - rest + j, None, j - w_lag, open_half, half_tiles)
            return 0

        lax.fori_loop(w_lag, rest, b_and_w, 0)
        for c in (n - 2, n - 1):
            for copy in keep_d(c):
                copy.wait()

        @pl.when(odd(done) == 1)
        def _():
            open_half(done)
            for tile in half_tiles:
                tile(done)

        def open_whole(m):
            with jax.named_scope("wait_w"):
                for w in (2 * m, 2 * m + 1):
                    for copy in fetch_w(w):
                        copy.wait()

        def whole_w(m, _):
            open_whole(m)
            fetch_pair(2 * m + 2)
            with jax.named_scope("WW"):
                for i, j in ((i, j) for i in range(3) for j in range(per)):
                    w_add(acc.at[i * per + j], term_of(i, m, 2 * odd(m) + j // (per // 2), j % (per // 2)))
            return 0

        lax.fori_loop(half_of(done + 1), micro - 1, whole_w, 0)

        m = micro - 1
        open_whole(m)

        def finish(i, take):
            for j in range(per):
                take(j, (acc[i * per + j] + rounded(term_of(i, m, 2 * odd(m) + j // (per // 2), j % (per // 2)))).astype(bf16))

        def take_down(j, v):
            h_ring[j] = v

        def take_gate(j, v):
            o_gate[0, :, j * 256 : (j + 1) * 256] = v

        def take_up(j, v):
            o_up[0, :, j * 256 : (j + 1) * 256] = v

        finish(2, take_down)
        finish(0, take_gate)
        for j in range(per):
            transpose_into(o_down.at[0, pl.ds(j * 256, 256), :], h_ring.at[j], rows, 256)
        finish(1, take_up)

    held = pltpu.VMEM((2, ff, CHUNK), f32)
    pl.run_scoped(phase_w, held, held, pltpu.VMEM((3 * per, rows, 256), f32), pltpu.VMEM((4, 3, 2, half, CHUNK), bf16))

    @pl.when(me < stages - 1)
    def _():
        def sent(c, _):
            send_f(c).wait_send()
            return 0

        lax.fori_loop(n - f_places, n, sent, 0)

    @pl.when(me > 0)
    def _():
        def sent(c, _):
            send_b(c).wait_send()
            return 0

        lax.fori_loop(n - b_places, n, sent, 0)


def solution(mesh):
    stages = mesh.shape["pp"]

    def step(x, dy, w_gate, w_up, w_down):
        micro, d = x.shape[0], x.shape[2]
        ff = w_gate.shape[2]
        n = 2 * micro
        hbm = pl.BlockSpec(memory_space=pltpu.HBM)
        out = pltpu.VMEM((1, d, ff), bf16)
        kept = jax.ShapeDtypeStruct((n, ff, CHUNK), f32)
        paired = jax.ShapeDtypeStruct((micro, 2, ff, CHUNK), bf16)
        dma = pltpu.SemaphoreType.DMA
        d_gate, d_up, d_down, *_ = pl.pallas_call(
            functools.partial(kernel, stages, micro),
            out_shape=[out, out, pltpu.VMEM((1, ff, d), bf16), kept, kept, paired, paired, paired],
            in_specs=[hbm] * 5,
            out_specs=[pl.BlockSpec(memory_space=pltpu.VMEM)] * 3 + [hbm] * 5,
            scratch_shapes=[
                pltpu.VMEM((n, d, CHUNK), bf16),
                pltpu.VMEM((n, d, CHUNK), bf16),
                pltpu.VMEM((2, ff, CHUNK), bf16),
                pltpu.VMEM((2, ff, CHUNK), bf16),
                pltpu.VMEM((SENDS, d, CHUNK), bf16),
                pltpu.VMEM((d, ff), bf16),
                pltpu.VMEM((d, ff), bf16),
                pltpu.VMEM((ff, d), bf16),
                dma((n,)),
                dma((n,)),
                dma((SENDS,)),
                dma((3, 2)),
                dma((2, 2)),
                dma((2, 2)),
                dma((4, 3)),
                dma((5,)),
            ],
            compiler_params=pltpu.CompilerParams(collective_id=0, has_side_effects=True, vmem_limit_bytes=61100000),
        )(x, dy, w_gate, w_up, w_down)
        return d_gate, d_up, d_down

    return jax.shard_map(
        step,
        mesh=mesh,
        in_specs=(P("rep", None, None),) * 2 + (P("pp", None, None),) * 3,
        out_specs=(P(("rep", "pp"), None, None),) * 3,
        check_vma=False,
    )
```
